32 devices in a mesh: gz: 4 (over y, core), gy: 2 (over x), gx: 4 (over z).
Axes of the slice: x: 2, y: 2, z: 4, core: 2. Of those that a mesh axis runs over, the one named last changes fastest.
Arguments:
- positions: float32 [3, 4, 4, 32, 128], P(None, 'gx', 'gy', 'gz'), may hold values from 0 to 1
- counts: int32 [4, 4, 32], P('gx', 'gy', 'gz'), may hold values from 104 to 128
Outputs:
- energy: float32 [4, 4, 32, 128], P('gx', 'gy', 'gz')
- forces: float32 [3, 4, 4, 32, 128], P(None, 'gx', 'gy', 'gz')
The draws below stay inside these ranges and needn't reach their ends.
Inputs may be any that keep to these rules, and one draw needn't show every extreme that they name: `counts`: slot k of a cell holds an atom exactly when k < its count; positions of other slots are not used.
All inputs are finite; a program needn't handle non-finite values.
Results may differ from the reference program's by a relative error of at most 0.0003.
Values sent between devices are 32-bit elements; how exact they have to be, the bound alone decides.
A program may use at most 64 MiB of HBM per device.

```python
import jax
import jax.numpy as jnp
from jax import lax

S = 128
NX = 4
NY = 4
NZ = 32


def touch_ends(result, own_key, smallest, top_value):
    dims = result.shape
    index_at = [jax.random.randint(jax.random.fold_in(own_key, axis), (), 0, dims[axis]) for axis in range(len(dims))]
    result = result.at[tuple(index_at)].set(smallest)
    longest = dims.index(max(dims))
    index_at[longest] = (index_at[longest] + 1) % dims[longest]
    return result.at[tuple(index_at)].set(top_value)


def block_scale(key, extent, shards, least, high):
    level = 1.0
    for dim, blocks in shards:
        steps = jax.random.uniform(jax.random.fold_in(jax.random.fold_in(key, 6), dim), (blocks,), jnp.float32, least / len(shards), high / len(shards))
        level = level * jnp.repeat(jnp.exp(steps), extent[dim] // blocks).reshape((-1,) + (1,) * (len(extent) - 1 - dim))
    return level


def setup_inputs(seed: int = 0) -> dict:
    arg_keys = jax.random.split(jax.random.key(seed), 3)
    return {
        "positions": jnp.clip(1.0 * jax.random.uniform(arg_keys[0], (3, NX, NY, NZ, S), jnp.float32) ** block_scale(arg_keys[0], (3, NX, NY, NZ, S), ((1, 4), (2, 2), (3, 4)), -0.2, 0.2), 0.0, 1.0),
        "counts": touch_ends(jax.random.randint(arg_keys[1], (NX, NY, NZ), S * 13 // 16, S + 1), jax.random.fold_in(arg_keys[1], 1), S * 13 // 16, S).astype(jnp.int32),
    }


SENTINEL = 4.0
PAIR_SCALE = 0.02
EMBED_SCALE = 0.2
CUTOFF_SQUARED = 0.25
FORCE_SCALE = 8.0
neighbour_offsets = [(step_x, step_y, step_z) for step_x in (-1, 0, 1) for step_y in (-1, 0, 1) for step_z in (-1, 0, 1)]

def pair_geometry(own_cells, far_cells, offset):
    deltas = []
    for component in range(3):
        deltas.append(far_cells[component][..., None, :] - own_cells[component][..., :, None] + offset[component])
    return deltas

def density_terms(own_cells, far_cells, offset, itself):
    deltas = pair_geometry(own_cells, far_cells, offset)
    squared = deltas[0] * deltas[0] + deltas[1] * deltas[1] + deltas[2] * deltas[2]
    weight = jnp.maximum(1.0 - squared / CUTOFF_SQUARED, 0.0)
    square = weight * weight
    if itself:
        slot_count = own_cells.shape[-1]
        square = jnp.where(jnp.eye(slot_count, dtype=bool), 0.0, square)
    return (lax.optimization_barrier(jnp.sum(square, -1)), lax.optimization_barrier(jnp.sum(PAIR_SCALE * (square * square - 2.0 * square), -1)))

def force_terms(own_cells, far_cells, own_fp, far_fp, offset):
    deltas = pair_geometry(own_cells, far_cells, offset)
    squared = deltas[0] * deltas[0] + deltas[1] * deltas[1] + deltas[2] * deltas[2]
    weight = jnp.maximum(1.0 - squared / CUTOFF_SQUARED, 0.0)
    factor = (own_fp[..., :, None] + far_fp[..., None, :]) * (-2.0 * weight) + 4.0 * PAIR_SCALE * weight * (1.0 - weight * weight)
    return jnp.stack([FORCE_SCALE * lax.optimization_barrier(jnp.sum(factor * delta, -1)) for delta in deltas])

def neighbour(field, column, step_x, step_y, step_z):
    cells_x = field.shape[1]
    slab = lax.dynamic_index_in_dim(field, (column + step_x) % cells_x, 1, keepdims=False)
    return jnp.roll(slab, (-step_y, -step_z), axis=(1, 2))

def reference(positions, counts):
    slot_count = positions.shape[-1]
    occupied = jnp.arange(slot_count, dtype=jnp.int32) < counts[..., None]
    seated = jnp.where(occupied[None], positions, SENTINEL)
    cells_x = seated.shape[1]
    columns = jnp.arange(cells_x, dtype=jnp.int32)

    def slab_density(column):
        own_cells = lax.dynamic_index_in_dim(seated, column, 1, keepdims=False)
        rho_sum = jnp.zeros(own_cells.shape[1:], own_cells.dtype)
        pair_sum = jnp.zeros(own_cells.shape[1:], own_cells.dtype)
        for step_x, step_y, step_z in neighbour_offsets:
            far_cells = neighbour(seated, column, step_x, step_y, step_z)
            itself = step_x == 0 and step_y == 0 and (step_z == 0)
            rho_part, pair_part = density_terms(own_cells, far_cells, (step_x, step_y, step_z), itself)
            rho_sum = rho_sum + rho_part
            pair_sum = pair_sum + pair_part
        return jnp.stack([rho_sum, pair_sum])
    density = lax.map(slab_density, columns)
    rho_sum = density[:, 0]
    pair_sum = density[:, 1]
    fprime = -0.5 * EMBED_SCALE * lax.rsqrt(rho_sum + 1.0)
    energy = jnp.where(occupied, -EMBED_SCALE * jnp.sqrt(rho_sum + 1.0) + 0.5 * pair_sum, 0.0)
    fp_field = fprime[None]

    def slab_force(column):
        own_cells = lax.dynamic_index_in_dim(seated, column, 1, keepdims=False)
        own_fp = lax.dynamic_index_in_dim(fp_field, column, 1, keepdims=False)[0]
        pushes = jnp.zeros(own_cells.shape, own_cells.dtype)
        for step_x, step_y, step_z in neighbour_offsets:
            far_cells = neighbour(seated, column, step_x, step_y, step_z)
            far_fp = neighbour(fp_field, column, step_x, step_y, step_z)[0]
            pushes = pushes + force_terms(own_cells, far_cells, own_fp, far_fp, (step_x, step_y, step_z))
        return pushes
    forces = jnp.moveaxis(lax.map(slab_force, columns), 0, 1)
    forces = jnp.where(occupied[None], forces, 0.0)
    return (energy, forces)
```

```python
import functools

import jax
import jax.numpy as jnp
from jax import lax
from jax.experimental import pallas as pl
from jax.experimental.pallas import tpu as pltpu
from jax.sharding import PartitionSpec as P

SENTINEL = 4.0
PAIR_SCALE = 0.02
EMBED_SCALE = 0.2
CUTOFF_SQUARED = 0.25
FORCE_SCALE = 8.0
FAR = -1.0e6
ROWS = 8


def with_halo(block, sides, width):
    for axis, dim in sides:
        count = lax.axis_size(axis)
        forward = [(i, (i + 1) % count) for i in range(count)]
        backward = [(target, source) for source, target in forward]
        low = lax.ppermute(
            lax.slice_in_dim(block, block.shape[dim] - width, None, axis=dim), axis, forward
        )
        high = lax.ppermute(lax.slice_in_dim(block, 0, width, axis=dim), axis, backward)
        block = jnp.concatenate([low, block, high], axis=dim)
    return block


def split(value):
    first = value.astype(jnp.bfloat16).astype(jnp.float32)
    rest = value - first
    second = rest.astype(jnp.bfloat16).astype(jnp.float32)
    return first, second, rest - second


def far_rows(tile):
    b1, b2, b3 = split(tile)
    return jnp.concatenate([b1, b2, b1, b2, b3, b1], axis=0)


def own_rows(tile):
    a1, a2, a3 = split(tile)
    return jnp.concatenate([a1, a1, a2, a2, a1, a3], axis=0)


def place(index, sizes):
    return index // (sizes[1] * sizes[2]), index // sizes[2] % sizes[1], index % sizes[2]


def density_kernel(far_ref, own_ref, out_ref, turned):
    wide = far_ref.shape[:3]
    sizes = own_ref.shape[:3]
    slots = far_ref.shape[-1]

    def prepare(index, carry):
        x, y, z = place(index, wide)
        turned[x, y, z] = far_rows(far_ref[x, y, z]).T.astype(jnp.bfloat16)
        return carry

    lax.fori_loop(0, wide[0] * wide[1] * wide[2], prepare, 0, unroll=4)

    def cell(index, carry):
        x, y, z = place(index, sizes)
        own = own_rows(own_ref[x, y, z]).astype(jnp.bfloat16)
        rho = jnp.zeros((ROWS, slots), jnp.float32)
        quartic = jnp.zeros((ROWS, slots), jnp.float32)
        for dx in range(3):
            for dy in range(3):
                for dz in range(3):
                    w = jnp.dot(
                        turned[x + dx, y + dy, z + dz], own, preferred_element_type=jnp.float32
                    )
                    w = jnp.maximum(w, 0.0)
                    s = w * w
                    q = s * s
                    rho = rho + jnp.sum(s.reshape(-1, ROWS, slots), axis=0)
                    quartic = quartic + jnp.sum(q.reshape(-1, ROWS, slots), axis=0)
        rho = jnp.sum(rho, axis=0, keepdims=True) - 1.0
        quartic = jnp.sum(quartic, axis=0, keepdims=True) - 1.0
        row = lax.broadcasted_iota(jnp.int32, (ROWS, slots), 0)
        out_ref[x, y, z] = jnp.where(row == 0, rho, quartic)
        return carry

    lax.fori_loop(0, sizes[0] * sizes[1] * sizes[2], cell, 0)


def force_kernel(far_ref, own_ref, gain_ref, out_ref, turned, flat):
    wide = far_ref.shape[:3]
    sizes = own_ref.shape[:3]
    slots = far_ref.shape[-1]

    def prepare(index, carry):
        x, y, z = place(index, wide)
        b1, b2, b3 = split(far_ref[x, y, z])
        turned[x, y, z] = jnp.concatenate([b1, b2, b1, b2, b3, b1], axis=0).T.astype(jnp.bfloat16)
        flat[x, y, z] = jnp.concatenate([b1, b2, b3, jnp.zeros_like(b1)], axis=0).astype(
            jnp.bfloat16
        )
        return carry

    lax.fori_loop(0, wide[0] * wide[1] * wide[2], prepare, 0, unroll=4)

    def cell(index, carry):
        x, y, z = place(index, sizes)
        tile = own_ref[x, y, z]
        own = jnp.concatenate([own_rows(tile), own_rows(gain_ref[x, y, z])], axis=1).astype(
            jnp.bfloat16
        )
        total = jnp.zeros((4 * ROWS, slots), jnp.float32)
        for dx in range(3):
            for dy in range(3):
                for dz in range(3):
                    both = jnp.dot(
                        turned[x + dx, y + dy, z + dz], own, preferred_element_type=jnp.float32
                    )
                    w = jnp.maximum(both[:, :slots], 0.0)
                    f = w * (both[:, slots:] - w * w)
                    high = f.astype(jnp.bfloat16)
                    low = (f - high.astype(jnp.float32)).astype(jnp.bfloat16)
                    rows = flat[x + dx, y + dy, z + dz]
                    total = total + jnp.dot(rows, high, preferred_element_type=jnp.float32)
                    total = total + jnp.dot(rows, low, preferred_element_type=jnp.float32)
        total = total[:ROWS] + total[ROWS : 2 * ROWS] + total[2 * ROWS : 3 * ROWS]
        scale = FORCE_SCALE * 4.0 * PAIR_SCALE
        out_ref[x, y, z] = scale * (total - 0.125 * tile * total[4:5])
        return carry

    lax.fori_loop(0, sizes[0] * sizes[1] * sizes[2], cell, 0)


def per_device(positions, counts):
    slots = positions.shape[-1]
    sizes = positions.shape[1:4]
    wide = tuple(size + 2 for size in sizes)
    occupied = jnp.arange(slots, dtype=jnp.int32) < counts[..., None]
    seated = jnp.where(occupied[None], positions, SENTINEL)
    block = with_halo(seated, (("gz", 3), ("gy", 2), ("gx", 1)), 1)
    filled = block[0] < 2.0
    coords = []
    for component in range(3):
        steps = lax.broadcasted_iota(jnp.float32, wide, component) - 0.5 * wide[component]
        coords.append(jnp.where(filled, block[component] + steps[..., None], 0.0))
    near = 4.0 * (coords[0] * coords[0] + coords[1] * coords[1] + coords[2] * coords[2])
    one = jnp.ones_like(near)
    zero = jnp.zeros_like(near)
    inner = tuple(slice(1, 1 + size) for size in sizes)
    far_density = jnp.stack(
        coords + [jnp.where(filled, -near, FAR), one, zero, zero, zero], axis=3
    )
    own = jnp.stack(
        [8.0 * c[inner] for c in coords]
        + [one[inner], 1.0 - near[inner], zero[inner], zero[inner], zero[inner]],
        axis=3,
    )
    depth = 6 * ROWS
    sums = pl.pallas_call(
        density_kernel,
        out_shape=jax.ShapeDtypeStruct(sizes + (ROWS, slots), jnp.float32),
        in_specs=[pl.BlockSpec(memory_space=pltpu.VMEM)] * 2,
        out_specs=pl.BlockSpec(memory_space=pltpu.VMEM),
        scratch_shapes=[pltpu.VMEM(wide + (slots, depth), jnp.bfloat16)],
        name="density",
    )(far_density, own)
    rho_sum = jnp.where(occupied, sums[..., 0, :], 0.0)
    pair_sum = PAIR_SCALE * (sums[..., 1, :] - 2.0 * rho_sum)
    fprime = -0.5 * EMBED_SCALE * lax.rsqrt(rho_sum + 1.0)
    gain = 0.5 - fprime * (0.5 / PAIR_SCALE)
    gain_block = with_halo(gain, (("gz", 2), ("gy", 1), ("gx", 0)), 1)
    far_force = jnp.stack(
        coords + [jnp.where(filled, -near, FAR), one, gain_block, zero, zero], axis=3
    )
    pad = zero[inner]
    gain_own = jnp.stack([pad, pad, pad, pad, gain, one[inner], pad, pad], axis=3)
    pushes = pl.pallas_call(
        force_kernel,
        out_shape=jax.ShapeDtypeStruct(sizes + (ROWS, slots), jnp.float32),
        in_specs=[pl.BlockSpec(memory_space=pltpu.VMEM)] * 3,
        out_specs=pl.BlockSpec(memory_space=pltpu.VMEM),
        scratch_shapes=[
            pltpu.VMEM(wide + (slots, depth), jnp.bfloat16),
            pltpu.VMEM(wide + (4 * ROWS, slots), jnp.bfloat16),
        ],
        name="force",
    )(far_force, own, gain_own)
    energy = jnp.where(occupied, -EMBED_SCALE * jnp.sqrt(rho_sum + 1.0) + 0.5 * pair_sum, 0.0)
    forces = jnp.moveaxis(pushes[..., :3, :], 3, 0)
    forces = jnp.where(occupied[None], forces, 0.0)
    return (energy, forces)


def solution(mesh):
    placed = (P(None, "gx", "gy", "gz", None), P("gx", "gy", "gz"))
    return jax.shard_map(
        per_device,
        mesh=mesh,
        in_specs=placed,
        out_specs=(P("gx", "gy", "gz", None), P(None, "gx", "gy", "gz", None)),
        check_vma=False,
    )
```

```python
import functools

import jax
import jax.numpy as jnp
from jax import lax
from jax.experimental import pallas as pl
from jax.experimental.pallas import tpu as pltpu
from jax.sharding import PartitionSpec as P

SENTINEL = 4.0
PAIR_SCALE = 0.02
EMBED_SCALE = 0.2
CUTOFF_SQUARED = 0.25
FORCE_SCALE = 8.0
FAR = -1.0e6
ROWS = 8


def with_halo(block, sides, width):
    for axis, dim in sides:
        count = lax.axis_size(axis)
        forward = [(i, (i + 1) % count) for i in range(count)]
        backward = [(target, source) for source, target in forward]
        low = lax.ppermute(
            lax.slice_in_dim(block, block.shape[dim] - width, None, axis=dim), axis, forward
        )
        high = lax.ppermute(lax.slice_in_dim(block, 0, width, axis=dim), axis, backward)
        block = jnp.concatenate([low, block, high], axis=dim)
    return block


def split(value):
    first = value.astype(jnp.bfloat16).astype(jnp.float32)
    rest = value - first
    second = rest.astype(jnp.bfloat16).astype(jnp.float32)
    return first, second, rest - second


def far_rows(tile):
    b1, b2, b3 = split(tile)
    return jnp.concatenate([b1, b2, b1, b2, b3, b1], axis=0)


def own_rows(tile):
    a1, a2, a3 = split(tile)
    return jnp.concatenate([a1, a1, a2, a2, a1, a3], axis=0)


def place(index, sizes):
    return index // (sizes[1] * sizes[2]), index // sizes[2] % sizes[1], index % sizes[2]


def groups(sizes):
    depth = 2 if sizes[2] % 2 == 0 else 1
    plan = []
    for dx in range(3):
        for jy in range(sizes[1] + 2):
            for jz in range(depth + 2):
                ys = [y for y in range(sizes[1]) if 0 <= jy - y <= 2]
                zs = [z for z in range(depth) if 0 <= jz - z <= 2]
                if len(ys) == sizes[1]:
                    runs = [(True, [(y, z) for z in zs for y in ys])]
                else:
                    runs = [(False, [(y, z) for z in zs]) for y in ys]
                plan.append((dx, jy, jz, runs))
    return depth, plan


def side_by_side(tiles, sizes, depth, layer_first):
    order = (
        [(y, z) for z in range(depth) for y in range(sizes[1])]
        if layer_first
        else [(y, z) for y in range(sizes[1]) for z in range(depth)]
    )
    return {key: at for at, key in enumerate(order)}, jnp.concatenate(
        [tiles[key] for key in order], axis=1
    )


def density_kernel(far_ref, own_ref, out_ref, turned):
    wide = far_ref.shape[:3]
    sizes = own_ref.shape[:3]
    slots = far_ref.shape[-1]
    depth, plan = groups(sizes)
    keys = [(y, z) for y in range(sizes[1]) for z in range(depth)]

    def prepare(index, carry):
        x, y, z = place(index, wide)
        turned[x, y, z] = far_rows(far_ref[x, y, z]).T.astype(jnp.bfloat16)
        return carry

    lax.fori_loop(0, wide[0] * wide[1] * wide[2], prepare, 0, unroll=4)

    def group(index, carry):
        steps = sizes[2] // depth
        x, z0 = index // steps, index % steps * depth
        tiles = {
            (y, z): own_rows(own_ref[x, y, z0 + z]).astype(jnp.bfloat16) for y, z in keys
        }
        packs = {flag: side_by_side(tiles, sizes, depth, flag) for flag in (True, False)}
        rho = {key: jnp.zeros((ROWS, slots), jnp.float32) for key in keys}
        quartic = {key: jnp.zeros((ROWS, slots), jnp.float32) for key in keys}
        for dx, jy, jz, runs in plan:
            rows = turned[x + dx, jy, z0 + jz]
            for flag, targets in runs:
                order, pack = packs[flag]
                start = order[targets[0]] * slots
                pack = pack[:, start : start + len(targets) * slots]
                both = jnp.dot(rows, pack, preferred_element_type=jnp.float32)
                for at, key in enumerate(targets):
                    w = jnp.maximum(both[:, at * slots : (at + 1) * slots], 0.0)
                    s = w * w
                    q = s * s
                    rho[key] = rho[key] + jnp.sum(s.reshape(-1, ROWS, slots), axis=0)
                    quartic[key] = quartic[key] + jnp.sum(q.reshape(-1, ROWS, slots), axis=0)
        row = lax.broadcasted_iota(jnp.int32, (ROWS, slots), 0)
        for key in keys:
            first = jnp.sum(rho[key], axis=0, keepdims=True) - 1.0
            second = jnp.sum(quartic[key], axis=0, keepdims=True) - 1.0
            out_ref[x, key[0], z0 + key[1]] = jnp.where(row == 0, first, second)
        return carry

    lax.fori_loop(0, sizes[0] * (sizes[2] // depth), group, 0)


def force_kernel(far_ref, own_ref, gain_ref, out_ref, turned, flat, column):
    wide = far_ref.shape[:3]
    sizes = own_ref.shape[:3]
    slots = far_ref.shape[-1]
    depth, plan = groups(sizes)
    keys = [(y, z) for y in range(sizes[1]) for z in range(depth)]

    def prepare(index, carry):
        x, y, z = place(index, wide)
        tile = far_ref[x, y, z]
        b1, b2, b3 = split(tile)
        across = jnp.concatenate([b1, b2, b1, b2, b3, b1, tile], axis=0).T
        turned[x, y, z] = across[:, : 6 * ROWS].astype(jnp.bfloat16)
        column[x, y, z] = across[:, 6 * ROWS + 5 : 6 * ROWS + 6]
        rows = jnp.concatenate([b1, b2, b3, jnp.zeros_like(b1)], axis=0).astype(jnp.bfloat16)
        flat[x, y, z] = jnp.concatenate([rows, rows], axis=1)
        return carry

    lax.fori_loop(0, wide[0] * wide[1] * wide[2], prepare, 0, unroll=4)

    def group(index, carry):
        steps = sizes[2] // depth
        x, z0 = index // steps, index % steps * depth
        tiles = {
            (y, z): own_rows(own_ref[x, y, z0 + z]).astype(jnp.bfloat16) for y, z in keys
        }
        packs = {flag: side_by_side(tiles, sizes, depth, flag) for flag in (True, False)}
        gains = {(y, z): gain_ref[x, y, z0 + z] for y, z in keys}
        total = {key: jnp.zeros((4 * ROWS, slots), jnp.float32) for key in keys}
        for dx, jy, jz, runs in plan:
            rows = turned[x + dx, jy, z0 + jz]
            moments = flat[x + dx, jy, z0 + jz]
            far_gain = jnp.broadcast_to(column[x + dx, jy, z0 + jz], (slots, slots))
            for flag, targets in runs:
                order, pack = packs[flag]
                start = order[targets[0]] * slots
                pack = pack[:, start : start + len(targets) * slots]
                both = jnp.dot(rows, pack, preferred_element_type=jnp.float32)
                highs, lows = [], []
                for at, key in enumerate(targets):
                    w = jnp.maximum(both[:, at * slots : (at + 1) * slots], 0.0)
                    f = w * ((far_gain + gains[key]) - w * w)
                    high = f.astype(jnp.bfloat16)
                    highs.append(high)
                    lows.append((f - high.astype(jnp.float32)).astype(jnp.bfloat16))
                stacked = jnp.concatenate(
                    [jnp.concatenate(highs, axis=1), jnp.concatenate(lows, axis=1)], axis=0
                )
                part = jnp.dot(moments, stacked, preferred_element_type=jnp.float32)
                for at, key in enumerate(targets):
                    total[key] = total[key] + part[:, at * slots : (at + 1) * slots]
        scale = FORCE_SCALE * 4.0 * PAIR_SCALE
        for key in keys:
            whole = total[key][:ROWS] + total[key][ROWS : 2 * ROWS] + total[key][2 * ROWS : 3 * ROWS]
            tile = own_ref[x, key[0], z0 + key[1]]
            out_ref[x, key[0], z0 + key[1]] = scale * (whole - 0.125 * tile * whole[4:5])
        return carry

    lax.fori_loop(0, sizes[0] * (sizes[2] // depth), group, 0)


def per_device(positions, counts):
    slots = positions.shape[-1]
    sizes = positions.shape[1:4]
    wide = tuple(size + 2 for size in sizes)
    occupied = jnp.arange(slots, dtype=jnp.int32) < counts[..., None]
    seated = jnp.where(occupied[None], positions, SENTINEL)
    block = with_halo(seated, (("gz", 3), ("gy", 2), ("gx", 1)), 1)
    filled = block[0] < 2.0
    coords = []
    for component in range(3):
        steps = lax.broadcasted_iota(jnp.float32, wide, component) - 0.5 * wide[component]
        coords.append(jnp.where(filled, block[component] + steps[..., None], 0.0))
    near = 4.0 * (coords[0] * coords[0] + coords[1] * coords[1] + coords[2] * coords[2])
    one = jnp.ones_like(near)
    zero = jnp.zeros_like(near)
    inner = tuple(slice(1, 1 + size) for size in sizes)
    far_density = jnp.stack(
        coords + [jnp.where(filled, -near, FAR), one, zero, zero, zero], axis=3
    )
    own = jnp.stack(
        [8.0 * c[inner] for c in coords]
        + [one[inner], 1.0 - near[inner], zero[inner], zero[inner], zero[inner]],
        axis=3,
    )
    depth = 6 * ROWS
    sums = pl.pallas_call(
        density_kernel,
        out_shape=jax.ShapeDtypeStruct(sizes + (ROWS, slots), jnp.float32),
        in_specs=[pl.BlockSpec(memory_space=pltpu.VMEM)] * 2,
        out_specs=pl.BlockSpec(memory_space=pltpu.VMEM),
        scratch_shapes=[pltpu.VMEM(wide + (slots, depth), jnp.bfloat16)],
        name="density",
    )(far_density, own)
    rho_sum = jnp.where(occupied, sums[..., 0, :], 0.0)
    pair_sum = PAIR_SCALE * (sums[..., 1, :] - 2.0 * rho_sum)
    fprime = -0.5 * EMBED_SCALE * lax.rsqrt(rho_sum + 1.0)
    gain = 0.5 - fprime * (0.5 / PAIR_SCALE)
    gain_block = with_halo(gain, (("gz", 2), ("gy", 1), ("gx", 0)), 1)
    far_force = jnp.stack(
        coords + [jnp.where(filled, -near, FAR), one, gain_block, zero, zero], axis=3
    )
    gain_own = gain[..., None, :]
    pushes = pl.pallas_call(
        force_kernel,
        out_shape=jax.ShapeDtypeStruct(sizes + (ROWS, slots), jnp.float32),
        in_specs=[pl.BlockSpec(memory_space=pltpu.VMEM)] * 3,
        out_specs=pl.BlockSpec(memory_space=pltpu.VMEM),
        scratch_shapes=[
            pltpu.VMEM(wide + (slots, depth), jnp.bfloat16),
            pltpu.VMEM(wide + (4 * ROWS, 2 * slots), jnp.bfloat16),
            pltpu.VMEM(wide + (slots, 1), jnp.float32),
        ],
        name="force",
    )(far_force, own, gain_own)
    energy = jnp.where(occupied, -EMBED_SCALE * jnp.sqrt(rho_sum + 1.0) + 0.5 * pair_sum, 0.0)
    forces = jnp.moveaxis(pushes[..., :3, :], 3, 0)
    forces = jnp.where(occupied[None], forces, 0.0)
    return (energy, forces)


def solution(mesh):
    placed = (P(None, "gx", "gy", "gz", None), P("gx", "gy", "gz"))
    return jax.shard_map(
        per_device,
        mesh=mesh,
        in_specs=placed,
        out_specs=(P("gx", "gy", "gz", None), P(None, "gx", "gy", "gz", None)),
        check_vma=False,
    )
```

```python
import functools

import jax
import jax.numpy as jnp
from jax import lax
from jax.experimental import pallas as pl
from jax.experimental.pallas import tpu as pltpu
from jax.sharding import PartitionSpec as P

SENTINEL = 4.0
PAIR_SCALE = 0.02
EMBED_SCALE = 0.2
CUTOFF_SQUARED = 0.25
FORCE_SCALE = 8.0
FAR = -1.0e6
ROWS = 8


def split(value):
    first = value.astype(jnp.bfloat16).astype(jnp.float32)
    rest = value - first
    second = rest.astype(jnp.bfloat16).astype(jnp.float32)
    return first, second, rest - second


def far_rows(tile):
    b1, b2, b3 = split(tile)
    return jnp.concatenate([b1, b2, b1, b2, b3, b1], axis=0)


def own_rows(tile):
    a1, a2, a3 = split(tile)
    return jnp.concatenate([a1, a1, a2, a2, a1, a3], axis=0)


def place(index, sizes):
    return index // (sizes[1] * sizes[2]), index // sizes[2] % sizes[1], index % sizes[2]


def groups(sizes):
    depth = 2 if sizes[2] % 2 == 0 else 1
    plan = []
    for dx in range(3):
        for jy in range(sizes[1] + 2):
            for jz in range(depth + 2):
                ys = [y for y in range(sizes[1]) if 0 <= jy - y <= 2]
                zs = [z for z in range(depth) if 0 <= jz - z <= 2]
                if len(ys) == sizes[1]:
                    runs = [(True, [(y, z) for z in zs for y in ys])]
                else:
                    runs = [(False, [(y, z) for z in zs]) for y in ys]
                plan.append((dx, jy, jz, runs))
    return depth, plan


def side_by_side(tiles, sizes, depth, layer_first):
    order = (
        [(y, z) for z in range(depth) for y in range(sizes[1])]
        if layer_first
        else [(y, z) for y in range(sizes[1]) for z in range(depth)]
    )
    return {key: at for at, key in enumerate(order)}, jnp.concatenate(
        [tiles[key] for key in order], axis=1
    )


def far_tile(tile, index, wide):
    row = lax.broadcasted_iota(jnp.int32, tile.shape, 0)
    steps = [at.astype(jnp.float32) - 0.5 * size for at, size in zip(index, wide)]
    shift = jnp.where(row == 0, steps[0], jnp.where(row == 1, steps[1], steps[2]))
    filled = tile[0:1] < 2.0
    coords = jnp.where(filled & (row < 3), tile + shift, 0.0)
    near = -4.0 * jnp.sum(coords * coords, axis=0, keepdims=True)
    upper = jnp.where(row == 3, jnp.where(filled, near, FAR), coords)
    lower = jnp.where(row == 0, 1.0, 0.0)
    return jnp.concatenate([upper, lower], axis=0)


def own_tile(tile, index, wide):
    row = lax.broadcasted_iota(jnp.int32, tile.shape, 0)
    far = far_tile(tile, index, wide)
    coords = jnp.where(row < 3, far[:4], 0.0)
    near = 4.0 * jnp.sum(coords * coords, axis=0, keepdims=True)
    upper = jnp.where(row == 3, 1.0, 8.0 * coords)
    lower = jnp.where(row == 0, 1.0 - near, 0.0)
    return jnp.concatenate([upper, lower], axis=0)


NAMES = ("gx", "gy", "gz")
DIRECTIONS = [
    (x, y, z) for x in (-1, 0, 1) for y in (-1, 0, 1) for z in (-1, 0, 1) if (x, y, z) != (0, 0, 0)
]


def device_at(counts, step):
    return {
        name: lax.rem(lax.axis_index(name) + (offset + count), count)
        for name, offset, count in zip(NAMES, step, counts)
    }


def meet(counts):
    barrier = pltpu.get_barrier_semaphore()
    partners = sorted({tuple(o % c for o, c in zip(step, counts)) for step in DIRECTIONS})
    for step in partners:
        pl.semaphore_signal(
            barrier,
            inc=1,
            device_id=device_at(counts, step),
            device_id_type=pl.DeviceIdType.MESH,
        )
    pl.semaphore_wait(barrier, len(partners))


def send_rims(counts, source, target, sent, landed):
    sizes = source.shape[:3]
    copies = []
    for at, step in enumerate(DIRECTIONS):
        here = tuple(
            pl.ds(0, size) if o == 0 else pl.ds(size - 1 if o > 0 else 0, 1)
            for o, size in zip(step, sizes)
        )
        there = tuple(
            pl.ds(1, size) if o == 0 else pl.ds(0 if o > 0 else size + 1, 1)
            for o, size in zip(step, sizes)
        )
        copy = pltpu.make_async_remote_copy(
            src_ref=source.at[here],
            dst_ref=target.at[there],
            send_sem=sent.at[at],
            recv_sem=landed.at[at],
            device_id=device_at(counts, step),
            device_id_type=pl.DeviceIdType.MESH,
        )
        copy.start()
        copies.append(copy)
    return copies


def kernel(
    counts,
    source,
    energy_ref,
    force_ref,
    ext,
    gain_own,
    gain_ext,
    turned,
    flat,
    column,
    sent,
    landed,
    gain_sent,
    gain_landed,
):
    sizes = source.shape[:3]
    wide = ext.shape[:3]
    slots = source.shape[-1]
    depth, plan = groups(sizes)
    keys = [(y, z) for y in range(sizes[1]) for z in range(depth)]
    steps = sizes[2] // depth
    cells = sizes[0] * sizes[1] * sizes[2]

    meet(counts)
    copies = send_rims(counts, source, ext, sent, landed)

    def inside(index, carry):
        x, y, z = place(index, sizes)
        ext[x + 1, y + 1, z + 1] = source[x, y, z]
        return carry

    lax.fori_loop(0, cells, inside, 0, unroll=4)
    for copy in copies:
        copy.wait()

    def prepare(index, carry):
        x, y, z = place(index, wide)
        b1, b2, b3 = split(far_tile(ext[x, y, z], (x, y, z), wide))
        across = jnp.concatenate([b1, b2, b1, b2, b3, b1], axis=0).T
        turned[x, y, z] = across.astype(jnp.bfloat16)
        rows = jnp.concatenate([b1, b2, b3, jnp.zeros_like(b1)], axis=0).astype(jnp.bfloat16)
        flat[x, y, z] = jnp.concatenate([rows, rows], axis=1)
        return carry

    lax.fori_loop(0, wide[0] * wide[1] * wide[2], prepare, 0, unroll=4)

    def group_tiles(x, z0):
        return {
            (y, z): own_tile(ext[x + 1, y + 1, z0 + z + 1], (x + 1, jnp.int32(y + 1), z0 + z + 1), wide)
            for y, z in keys
        }

    def group_packs(tiles):
        rows = {key: own_rows(tile).astype(jnp.bfloat16) for key, tile in tiles.items()}
        return {flag: side_by_side(rows, sizes, depth, flag) for flag in (True, False)}

    def density_group(index, carry):
        x, z0 = index // steps, index % steps * depth
        packs = group_packs(group_tiles(x, z0))
        rho = {key: jnp.zeros((ROWS, slots), jnp.float32) for key in keys}
        quartic = {key: jnp.zeros((ROWS, slots), jnp.float32) for key in keys}
        for dx, jy, jz, runs in plan:
            rows = turned[x + dx, jy, z0 + jz]
            for flag, targets in runs:
                order, pack = packs[flag]
                start = order[targets[0]] * slots
                pack = pack[:, start : start + len(targets) * slots]
                both = jnp.dot(rows, pack, preferred_element_type=jnp.float32)
                for at, key in enumerate(targets):
                    w = jnp.maximum(both[:, at * slots : (at + 1) * slots], 0.0)
                    s = w * w
                    q = s * s
                    rho[key] = rho[key] + jnp.sum(s.reshape(-1, ROWS, slots), axis=0)
                    quartic[key] = quartic[key] + jnp.sum(q.reshape(-1, ROWS, slots), axis=0)
        for y, z in keys:
            filled = ext[x + 1, y + 1, z0 + z + 1][0:1] < 2.0
            first = jnp.sum(rho[y, z], axis=0, keepdims=True) - 1.0
            second = jnp.sum(quartic[y, z], axis=0, keepdims=True) - 1.0
            first = jnp.where(filled, first, 0.0)
            pair_sum = PAIR_SCALE * (second - 2.0 * first)
            energy = -EMBED_SCALE * jnp.sqrt(first + 1.0) + 0.5 * pair_sum
            energy_ref[x, y, pl.ds(z0 + z, 1)] = jnp.where(filled, energy, 0.0)
            fprime = -0.5 * EMBED_SCALE * lax.rsqrt(first + 1.0)
            gain = 0.5 - fprime * (0.5 / PAIR_SCALE)
            gain_own[x, y, z0 + z] = gain
            gain_ext[x + 1, y + 1, z0 + z + 1] = gain
        return carry

    lax.fori_loop(0, sizes[0] * steps, density_group, 0)
    copies = send_rims(counts, gain_own, gain_ext, gain_sent, gain_landed)
    for copy in copies:
        copy.wait()

    def raise_gain(index, carry):
        x, y, z = place(index, wide)
        column[x, y, z] = jnp.broadcast_to(gain_ext[x, y, z], (ROWS, slots)).T[:, :1]
        return carry

    lax.fori_loop(0, wide[0] * wide[1] * wide[2], raise_gain, 0, unroll=4)

    def force_group(index, carry):
        x, z0 = index // steps, index % steps * depth
        tiles = group_tiles(x, z0)
        packs = group_packs(tiles)
        gains = {(y, z): gain_own[x, y, z0 + z] for y, z in keys}
        total = {key: jnp.zeros((4 * ROWS, slots), jnp.float32) for key in keys}
        for dx, jy, jz, runs in plan:
            rows = turned[x + dx, jy, z0 + jz]
            moments = flat[x + dx, jy, z0 + jz]
            far_gain = jnp.broadcast_to(column[x + dx, jy, z0 + jz], (slots, slots))
            for flag, targets in runs:
                order, pack = packs[flag]
                start = order[targets[0]] * slots
                pack = pack[:, start : start + len(targets) * slots]
                both = jnp.dot(rows, pack, preferred_element_type=jnp.float32)
                highs, lows = [], []
                for at, key in enumerate(targets):
                    w = jnp.maximum(both[:, at * slots : (at + 1) * slots], 0.0)
                    f = w * ((far_gain + gains[key]) - w * w)
                    high = f.astype(jnp.bfloat16)
                    highs.append(high)
                    lows.append((f - high.astype(jnp.float32)).astype(jnp.bfloat16))
                stacked = jnp.concatenate(
                    [jnp.concatenate(highs, axis=1), jnp.concatenate(lows, axis=1)], axis=0
                )
                part = jnp.dot(moments, stacked, preferred_element_type=jnp.float32)
                for at, key in enumerate(targets):
                    total[key] = total[key] + part[:, at * slots : (at + 1) * slots]
        scale = FORCE_SCALE * 4.0 * PAIR_SCALE
        for y, z in keys:
            parts = total[y, z]
            whole = parts[:ROWS] + parts[ROWS : 2 * ROWS] + parts[2 * ROWS : 3 * ROWS]
            filled = ext[x + 1, y + 1, z0 + z + 1][0:1] < 2.0
            push = scale * (whole - 0.125 * tiles[y, z] * whole[4:5])
            push = jnp.where(filled, push, 0.0)
            for component in range(3):
                force_ref[component, x, y, pl.ds(z0 + z, 1)] = push[component : component + 1]
        return carry

    lax.fori_loop(0, sizes[0] * steps, force_group, 0)


def per_device(mesh_counts, positions, counts):
    slots = positions.shape[-1]
    sizes = positions.shape[1:4]
    wide = tuple(size + 2 for size in sizes)
    occupied = jnp.arange(slots, dtype=jnp.int32) < counts[..., None]
    seated = jnp.where(occupied[None], positions, SENTINEL)
    source = jnp.stack([seated[0], seated[1], seated[2], jnp.zeros_like(seated[0])], axis=3)
    return pl.pallas_call(
        functools.partial(kernel, mesh_counts),
        out_shape=(
            jax.ShapeDtypeStruct(sizes + (slots,), jnp.float32),
            jax.ShapeDtypeStruct((3,) + sizes + (slots,), jnp.float32),
        ),
        in_specs=[pl.BlockSpec(memory_space=pltpu.VMEM)],
        out_specs=(pl.BlockSpec(memory_space=pltpu.VMEM),) * 2,
        scratch_shapes=[
            pltpu.VMEM(wide + (4, slots), jnp.float32),
            pltpu.VMEM(sizes + (1, slots), jnp.float32),
            pltpu.VMEM(wide + (1, slots), jnp.float32),
            pltpu.VMEM(wide + (slots, 6 * ROWS), jnp.bfloat16),
            pltpu.VMEM(wide + (4 * ROWS, 2 * slots), jnp.bfloat16),
            pltpu.VMEM(wide + (slots, 1), jnp.float32),
        ]
        + [pltpu.SemaphoreType.DMA((len(DIRECTIONS),))] * 4,
        compiler_params=pltpu.CompilerParams(collective_id=0, has_side_effects=True),
        name="atoms",
    )(source)


def solution(mesh):
    placed = (P(None, "gx", "gy", "gz", None), P("gx", "gy", "gz"))
    return jax.shard_map(
        functools.partial(per_device, tuple(mesh.shape[name] for name in NAMES)),
        mesh=mesh,
        in_specs=placed,
        out_specs=(P("gx", "gy", "gz", None), P(None, "gx", "gy", "gz", None)),
        check_vma=False,
    )
```

```python
import functools

import jax
import jax.numpy as jnp
from jax import lax
from jax.experimental import pallas as pl
from jax.experimental.pallas import tpu as pltpu
from jax.sharding import PartitionSpec as P

SENTINEL = 4.0
PAIR_SCALE = 0.02
EMBED_SCALE = 0.2
CUTOFF_SQUARED = 0.25
FORCE_SCALE = 8.0
FAR = -1.0e6
ROWS = 8


def split(value):
    first = value.astype(jnp.bfloat16).astype(jnp.float32)
    rest = value - first
    second = rest.astype(jnp.bfloat16).astype(jnp.float32)
    return first, second, rest - second


def far_rows(tile):
    b1, b2, b3 = split(tile)
    return jnp.concatenate([b1, b2, b1, b2, b3, b1], axis=0)


def own_rows(tile):
    a1, a2, a3 = split(tile)
    return jnp.concatenate([a1, a1, a2, a2, a1, a3], axis=0)


def place(index, sizes):
    return index // (sizes[1] * sizes[2]), index // sizes[2] % sizes[1], index % sizes[2]


def groups(sizes):
    depth = 2 if sizes[2] % 2 == 0 else 1
    plan = []
    for dx in range(3):
        for jy in range(sizes[1] + 2):
            for jz in range(depth + 2):
                ys = [y for y in range(sizes[1]) if 0 <= jy - y <= 2]
                zs = [z for z in range(depth) if 0 <= jz - z <= 2]
                if len(ys) == sizes[1]:
                    runs = [(True, [(y, z) for z in zs for y in ys])]
                else:
                    runs = [(False, [(y, z) for z in zs]) for y in ys]
                plan.append((dx, jy, jz, runs))
    return depth, plan


def side_by_side(tiles, sizes, depth, layer_first):
    order = (
        [(y, z) for z in range(depth) for y in range(sizes[1])]
        if layer_first
        else [(y, z) for y in range(sizes[1]) for z in range(depth)]
    )
    return {key: at for at, key in enumerate(order)}, jnp.concatenate(
        [tiles[key] for key in order], axis=1
    )


def far_tile(tile, index, wide):
    row = lax.broadcasted_iota(jnp.int32, tile.shape, 0)
    steps = [at.astype(jnp.float32) - 0.5 * size for at, size in zip(index, wide)]
    shift = jnp.where(row == 0, steps[0], jnp.where(row == 1, steps[1], steps[2]))
    filled = tile[0:1] < 2.0
    coords = jnp.where(filled & (row < 3), tile + shift, 0.0)
    near = -4.0 * jnp.sum(coords * coords, axis=0, keepdims=True)
    upper = jnp.where(row == 3, jnp.where(filled, near, FAR), coords)
    lower = jnp.where(row == 0, 1.0, 0.0)
    return jnp.concatenate([upper, lower], axis=0)


def own_tile(tile, index, wide):
    row = lax.broadcasted_iota(jnp.int32, tile.shape, 0)
    far = far_tile(tile, index, wide)
    coords = jnp.where(row < 3, far[:4], 0.0)
    near = 4.0 * jnp.sum(coords * coords, axis=0, keepdims=True)
    upper = jnp.where(row == 3, 1.0, 8.0 * coords)
    lower = jnp.where(row == 0, 1.0 - near, 0.0)
    return jnp.concatenate([upper, lower], axis=0)


NAMES = ("gx", "gy", "gz")
DIRECTIONS = [
    (x, y, z) for x in (-1, 0, 1) for y in (-1, 0, 1) for z in (-1, 0, 1) if (x, y, z) != (0, 0, 0)
]


def device_at(counts, step):
    return {
        name: lax.rem(lax.axis_index(name) + (offset + count), count)
        for name, offset, count in zip(NAMES, step, counts)
    }


def meet(counts):
    barrier = pltpu.get_barrier_semaphore()
    partners = sorted({tuple(o % c for o, c in zip(step, counts)) for step in DIRECTIONS})
    for step in partners:
        pl.semaphore_signal(
            barrier,
            inc=1,
            device_id=device_at(counts, step),
            device_id_type=pl.DeviceIdType.MESH,
        )
    pl.semaphore_wait(barrier, len(partners))


def send_rims(counts, source, target, sent, landed):
    sizes = source.shape[:3]
    copies = []
    for at, step in enumerate(DIRECTIONS):
        here = tuple(
            pl.ds(0, size) if o == 0 else pl.ds(size - 1 if o > 0 else 0, 1)
            for o, size in zip(step, sizes)
        )
        there = tuple(
            pl.ds(1, size) if o == 0 else pl.ds(0 if o > 0 else size + 1, 1)
            for o, size in zip(step, sizes)
        )
        copy = pltpu.make_async_remote_copy(
            src_ref=source.at[here],
            dst_ref=target.at[there],
            send_sem=sent.at[at],
            recv_sem=landed.at[at],
            device_id=device_at(counts, step),
            device_id_type=pl.DeviceIdType.MESH,
        )
        copy.start()
        copies.append(copy)
    return copies


def kernel(
    counts,
    source,
    energy_ref,
    force_ref,
    ext,
    gain_own,
    gain_ext,
    turned,
    flat,
    column,
    sent,
    landed,
    gain_sent,
    gain_landed,
):
    sizes = source.shape[:3]
    wide = ext.shape[:3]
    slots = source.shape[-1]
    depth, plan = groups(sizes)
    keys = [(y, z) for y in range(sizes[1]) for z in range(depth)]
    steps = sizes[2] // depth

    meet(counts)
    copies = send_rims(counts, source, ext, sent, landed)

    inner = tuple(slice(1, 1 + size) for size in sizes)
    ext[inner] = source[...]
    for copy in copies:
        copy.wait()

    def prepare(index, carry):
        x, y = index // wide[1], index % wide[1]
        for z in range(wide[2]):
            b1, b2, b3 = split(far_tile(ext[x, y, z], (x, y, jnp.int32(z)), wide))
            across = jnp.concatenate([b1, b2, b1, b2, b3, b1], axis=0).T
            turned[x, y, z] = across.astype(jnp.bfloat16)
            rows = jnp.concatenate([b1, b2, b3, jnp.zeros_like(b1)], axis=0).astype(jnp.bfloat16)
            flat[x, y, z] = jnp.concatenate([rows, rows], axis=1)
        return carry

    lax.fori_loop(0, wide[0] * wide[1], prepare, 0)

    def group_tiles(x, z0):
        return {
            (y, z): own_tile(ext[x + 1, y + 1, z0 + z + 1], (x + 1, jnp.int32(y + 1), z0 + z + 1), wide)
            for y, z in keys
        }

    def group_packs(tiles):
        rows = {key: own_rows(tile).astype(jnp.bfloat16) for key, tile in tiles.items()}
        return {flag: side_by_side(rows, sizes, depth, flag) for flag in (True, False)}

    def density_group(index, carry):
        x, z0 = index // steps, index % steps * depth
        packs = group_packs(group_tiles(x, z0))
        rho = {key: jnp.zeros((ROWS, slots), jnp.float32) for key in keys}
        quartic = {key: jnp.zeros((ROWS, slots), jnp.float32) for key in keys}
        for dx, jy, jz, runs in plan:
            rows = turned[x + dx, jy, z0 + jz]
            for flag, targets in runs:
                order, pack = packs[flag]
                start = order[targets[0]] * slots
                pack = pack[:, start : start + len(targets) * slots]
                both = jnp.dot(rows, pack, preferred_element_type=jnp.float32)
                for at, key in enumerate(targets):
                    w = jnp.maximum(both[:, at * slots : (at + 1) * slots], 0.0)
                    s = w * w
                    q = s * s
                    rho[key] = rho[key] + jnp.sum(s.reshape(-1, ROWS, slots), axis=0)
                    quartic[key] = quartic[key] + jnp.sum(q.reshape(-1, ROWS, slots), axis=0)
        for y, z in keys:
            filled = ext[x + 1, y + 1, z0 + z + 1][0:1] < 2.0
            first = jnp.sum(rho[y, z], axis=0, keepdims=True) - 1.0
            second = jnp.sum(quartic[y, z], axis=0, keepdims=True) - 1.0
            first = jnp.where(filled, first, 0.0)
            pair_sum = PAIR_SCALE * (second - 2.0 * first)
            energy = -EMBED_SCALE * jnp.sqrt(first + 1.0) + 0.5 * pair_sum
            energy_ref[x, y, pl.ds(z0 + z, 1)] = jnp.where(filled, energy, 0.0)
            fprime = -0.5 * EMBED_SCALE * lax.rsqrt(first + 1.0)
            gain = 0.5 - fprime * (0.5 / PAIR_SCALE)
            gain_own[x, y, z0 + z] = gain
            gain_ext[x + 1, y + 1, z0 + z + 1] = gain
        return carry

    lax.fori_loop(0, sizes[0] * steps, density_group, 0)
    copies = send_rims(counts, gain_own, gain_ext, gain_sent, gain_landed)
    for copy in copies:
        copy.wait()

    def raise_gain(index, carry):
        x, y = index // wide[1], index % wide[1]
        rows = [gain_ext[x, y, z] for z in range(wide[2])]
        rows += [jnp.zeros((1, slots), jnp.float32)] * (-wide[2] % ROWS)
        column[x, y, :, : len(rows)] = jnp.concatenate(rows, axis=0).T
        return carry

    lax.fori_loop(0, wide[0] * wide[1], raise_gain, 0, unroll=2)

    def force_group(index, carry):
        x, z0 = index // steps, index % steps * depth
        tiles = group_tiles(x, z0)
        packs = group_packs(tiles)
        gains = {(y, z): gain_own[x, y, z0 + z] for y, z in keys}
        total = {key: jnp.zeros((4 * ROWS, slots), jnp.float32) for key in keys}
        for dx, jy, jz, runs in plan:
            rows = turned[x + dx, jy, z0 + jz]
            moments = flat[x + dx, jy, z0 + jz]
            if jz == 0:
                lanes = pltpu.roll(column[x + dx, jy], slots - z0, 1)
            far_gain = jnp.broadcast_to(lanes[:, jz : jz + 1], (slots, slots))
            for flag, targets in runs:
                order, pack = packs[flag]
                start = order[targets[0]] * slots
                pack = pack[:, start : start + len(targets) * slots]
                both = jnp.dot(rows, pack, preferred_element_type=jnp.float32)
                highs, lows = [], []
                for at, key in enumerate(targets):
                    w = jnp.maximum(both[:, at * slots : (at + 1) * slots], 0.0)
                    f = w * ((far_gain + gains[key]) - w * w)
                    high = f.astype(jnp.bfloat16)
                    highs.append(high)
                    lows.append((f - high.astype(jnp.float32)).astype(jnp.bfloat16))
                stacked = jnp.concatenate(
                    [jnp.concatenate(highs, axis=1), jnp.concatenate(lows, axis=1)], axis=0
                )
                part = jnp.dot(moments, stacked, preferred_element_type=jnp.float32)
                for at, key in enumerate(targets):
                    total[key] = total[key] + part[:, at * slots : (at + 1) * slots]
        scale = FORCE_SCALE * 4.0 * PAIR_SCALE
        for y, z in keys:
            parts = total[y, z]
            whole = parts[:ROWS] + parts[ROWS : 2 * ROWS] + parts[2 * ROWS : 3 * ROWS]
            filled = ext[x + 1, y + 1, z0 + z + 1][0:1] < 2.0
            push = scale * (whole - 0.125 * tiles[y, z] * whole[4:5])
            push = jnp.where(filled, push, 0.0)
            for component in range(3):
                force_ref[component, x, y, pl.ds(z0 + z, 1)] = push[component : component + 1]
        return carry

    lax.fori_loop(0, sizes[0] * steps, force_group, 0)


def per_device(mesh_counts, positions, counts):
    slots = positions.shape[-1]
    sizes = positions.shape[1:4]
    wide = tuple(size + 2 for size in sizes)
    occupied = jnp.arange(slots, dtype=jnp.int32) < counts[..., None]
    seated = jnp.where(occupied[None], positions, SENTINEL)
    source = jnp.stack([seated[0], seated[1], seated[2], jnp.zeros_like(seated[0])], axis=3)
    return pl.pallas_call(
        functools.partial(kernel, mesh_counts),
        out_shape=(
            jax.ShapeDtypeStruct(sizes + (slots,), jnp.float32),
            jax.ShapeDtypeStruct((3,) + sizes + (slots,), jnp.float32),
        ),
        in_specs=[pl.BlockSpec(memory_space=pltpu.VMEM)],
        out_specs=(pl.BlockSpec(memory_space=pltpu.VMEM),) * 2,
        scratch_shapes=[
            pltpu.VMEM(wide + (4, slots), jnp.float32),
            pltpu.VMEM(sizes + (1, slots), jnp.float32),
            pltpu.VMEM(wide + (1, slots), jnp.float32),
            pltpu.VMEM(wide + (slots, 6 * ROWS), jnp.bfloat16),
            pltpu.VMEM(wide + (4 * ROWS, 2 * slots), jnp.bfloat16),
            pltpu.VMEM(wide[:2] + (slots, slots), jnp.float32),
        ]
        + [pltpu.SemaphoreType.DMA((len(DIRECTIONS),))] * 4,
        compiler_params=pltpu.CompilerParams(collective_id=0, has_side_effects=True),
        name="atoms",
    )(source)


def solution(mesh):
    placed = (P(None, "gx", "gy", "gz", None), P("gx", "gy", "gz"))
    return jax.shard_map(
        functools.partial(per_device, tuple(mesh.shape[name] for name in NAMES)),
        mesh=mesh,
        in_specs=placed,
        out_specs=(P("gx", "gy", "gz", None), P(None, "gx", "gy", "gz", None)),
        check_vma=False,
    )
```

```python
import functools

import jax
import jax.numpy as jnp
from jax import lax
from jax.experimental import pallas as pl
from jax.experimental.pallas import tpu as pltpu
from jax.sharding import PartitionSpec as P

SENTINEL = 4.0
PAIR_SCALE = 0.02
EMBED_SCALE = 0.2
CUTOFF_SQUARED = 0.25
FORCE_SCALE = 8.0
FAR = -1.0e6
ROWS = 8


def split(value):
    first = value.astype(jnp.bfloat16).astype(jnp.float32)
    rest = value - first
    second = rest.astype(jnp.bfloat16).astype(jnp.float32)
    return first, second, rest - second


def far_rows(tile):
    b1, b2, b3 = split(tile)
    return jnp.concatenate([b1, b2, b1, b2, b3, b1], axis=0)


def own_rows(tile):
    a1, a2, a3 = split(tile)
    return jnp.concatenate([a1, a1, a2, a2, a1, a3], axis=0)


def place(index, sizes):
    return index // (sizes[1] * sizes[2]), index // sizes[2] % sizes[1], index % sizes[2]


def groups(sizes):
    depth = 2 if sizes[2] % 2 == 0 else 1
    plan = []
    for dx in range(3):
        for jy in range(sizes[1] + 2):
            for jz in range(depth + 2):
                ys = [y for y in range(sizes[1]) if 0 <= jy - y <= 2]
                zs = [z for z in range(depth) if 0 <= jz - z <= 2]
                if len(ys) == sizes[1]:
                    runs = [(True, [(y, z) for z in zs for y in ys])]
                else:
                    runs = [(False, [(y, z) for z in zs]) for y in ys]
                plan.append((dx, jy, jz, runs))
    return depth, plan


def side_by_side(tiles, sizes, depth, layer_first):
    order = (
        [(y, z) for z in range(depth) for y in range(sizes[1])]
        if layer_first
        else [(y, z) for y in range(sizes[1]) for z in range(depth)]
    )
    return {key: at for at, key in enumerate(order)}, jnp.concatenate(
        [tiles[key] for key in order], axis=1
    )


def far_tile(tile, index, wide):
    row = lax.broadcasted_iota(jnp.int32, tile.shape, 0)
    steps = [at.astype(jnp.float32) - 0.5 * size for at, size in zip(index, wide)]
    shift = jnp.where(row == 0, steps[0], jnp.where(row == 1, steps[1], steps[2]))
    filled = tile[0:1] < 2.0
    coords = jnp.where(filled & (row < 3), tile + shift, 0.0)
    near = -4.0 * jnp.sum(coords * coords, axis=0, keepdims=True)
    upper = jnp.where(row == 3, jnp.where(filled, near, FAR), coords)
    lower = jnp.where(row == 0, 1.0, 0.0)
    return jnp.concatenate([upper, lower], axis=0)


def own_tile(tile, index, wide):
    row = lax.broadcasted_iota(jnp.int32, tile.shape, 0)
    far = far_tile(tile, index, wide)
    coords = jnp.where(row < 3, far[:4], 0.0)
    near = 4.0 * jnp.sum(coords * coords, axis=0, keepdims=True)
    upper = jnp.where(row == 3, 1.0, 8.0 * coords)
    lower = jnp.where(row == 0, 1.0 - near, 0.0)
    return jnp.concatenate([upper, lower], axis=0)


NAMES = ("gx", "gy", "gz")
DIRECTIONS = [(0, 0, 1), (0, 0, -1), (0, 1, 0), (0, -1, 0), (1, 0, 0), (-1, 0, 0)]
MESSAGES = 10


def device_at(counts, step):
    return {
        name: lax.rem(lax.axis_index(name) + (offset + count), count)
        for name, offset, count in zip(NAMES, step, counts)
    }


def meet(counts):
    barrier = pltpu.get_barrier_semaphore()
    partners = sorted({tuple(o % c for o, c in zip(step, counts)) for step in DIRECTIONS})
    for step in partners:
        pl.semaphore_signal(
            barrier,
            inc=1,
            device_id=device_at(counts, step),
            device_id_type=pl.DeviceIdType.MESH,
        )
    pl.semaphore_wait(barrier, len(partners))


def swap_rims(counts, block, ext, sent, landed, filling, column_work):
    sizes = block.shape[:3]
    low, high = pl.ds(0, 1), [pl.ds(size + 1, 1) for size in sizes]
    first, last = pl.ds(1, 1), [pl.ds(size, 1) for size in sizes]
    whole = pl.ds(0, sizes[2] + 2)
    inner = [pl.ds(1, size) for size in sizes]
    started = []

    def send(step, source, here, there):
        at = len(started)
        copy = pltpu.make_async_remote_copy(
            src_ref=source.at[here],
            dst_ref=ext.at[there],
            send_sem=sent.at[at],
            recv_sem=landed.at[at],
            device_id=device_at(counts, step),
            device_id_type=pl.DeviceIdType.MESH,
        )
        copy.start()
        started.append(copy)
        return copy

    flat = tuple(pl.ds(0, size) for size in sizes[:2])
    tops = [
        send((0, 0, 1), block, flat + (pl.ds(sizes[2] - 1, 1),), (inner[0], inner[1], low)),
        send((0, 0, -1), block, flat + (pl.ds(0, 1),), (inner[0], inner[1], high[2])),
    ]
    if filling is not None:
        filling.wait()
    for copy in tops:
        copy.wait_recv()
    sides = [
        send((0, 1, 0), ext, (inner[0], last[1], whole), (inner[0], low, whole)),
        send((0, -1, 0), ext, (inner[0], first, whole), (inner[0], high[1], whole)),
    ]
    slabs = [
        send((1, 0, 0), ext, (last[0], inner[1], whole), (low, inner[1], whole)),
        send((-1, 0, 0), ext, (first, inner[1], whole), (high[0], inner[1], whole)),
    ]
    column_work(sizes[0] * sizes[1], lambda i: (i // sizes[1] + 1, i % sizes[1] + 1))
    for copy in sides:
        copy.wait_recv()
    edges = []
    for row in (low, high[1]):
        edges.append(send((1, 0, 0), ext, (last[0], row, whole), (low, row, whole)))
        edges.append(send((-1, 0, 0), ext, (first, row, whole), (high[0], row, whole)))
    column_work(2 * sizes[0], lambda i: (i // 2 + 1, i % 2 * (sizes[1] + 1)))
    for copy in slabs:
        copy.wait_recv()
    column_work(2 * sizes[1], lambda i: (i % 2 * (sizes[0] + 1), i // 2 + 1))
    for copy in edges:
        copy.wait_recv()
    column_work(4, lambda i: (i % 2 * (sizes[0] + 1), i // 2 * (sizes[1] + 1)))
    for copy in started:
        copy.wait_send()


def kernel(
    counts,
    source,
    energy_ref,
    force_ref,
    ext,
    gain_own,
    gain_ext,
    turned,
    flat,
    column,
    sent,
    landed,
    gain_sent,
    gain_landed,
    filled_sem,
):
    sizes = source.shape[:3]
    wide = ext.shape[:3]
    slots = source.shape[-1]
    depth, plan = groups(sizes)
    keys = [(y, z) for y in range(sizes[1]) for z in range(depth)]
    steps = sizes[2] // depth

    inner = tuple(pl.ds(1, size) for size in sizes)
    filling = pltpu.make_async_copy(source, ext.at[inner], filled_sem.at[0])
    filling.start()
    meet(counts)

    def prepare(x, y):
        for z in range(wide[2]):
            b1, b2, b3 = split(far_tile(ext[x, y, z], (x, y, jnp.int32(z)), wide))
            across = jnp.concatenate([b1, b2, b1, b2, b3, b1], axis=0).T
            turned[x, y, z] = across.astype(jnp.bfloat16)
            rows = jnp.concatenate([b1, b2, b3, jnp.zeros_like(b1)], axis=0).astype(jnp.bfloat16)
            flat[x, y, z] = jnp.concatenate([rows, rows], axis=1)

    def looped(body):
        def work(count, where):
            def step(index, carry):
                body(*where(index))
                return carry

            lax.fori_loop(0, count, step, 0)

        return work

    swap_rims(counts, source, ext, sent, landed, filling, looped(prepare))

    def group_tiles(x, z0):
        return {
            (y, z): own_tile(ext[x + 1, y + 1, z0 + z + 1], (x + 1, jnp.int32(y + 1), z0 + z + 1), wide)
            for y, z in keys
        }

    def group_packs(tiles):
        rows = {key: own_rows(tile).astype(jnp.bfloat16) for key, tile in tiles.items()}
        return {flag: side_by_side(rows, sizes, depth, flag) for flag in (True, False)}

    def density_group(index, carry):
        x, z0 = index // steps, index % steps * depth
        packs = group_packs(group_tiles(x, z0))
        rho = {key: jnp.zeros((ROWS, slots), jnp.float32) for key in keys}
        quartic = {key: jnp.zeros((ROWS, slots), jnp.float32) for key in keys}
        for dx, jy, jz, runs in plan:
            rows = turned[x + dx, jy, z0 + jz]
            for flag, targets in runs:
                order, pack = packs[flag]
                start = order[targets[0]] * slots
                pack = pack[:, start : start + len(targets) * slots]
                both = jnp.dot(rows, pack, preferred_element_type=jnp.float32)
                for at, key in enumerate(targets):
                    w = jnp.maximum(both[:, at * slots : (at + 1) * slots], 0.0)
                    s = w * w
                    q = s * s
                    rho[key] = rho[key] + jnp.sum(s.reshape(-1, ROWS, slots), axis=0)
                    quartic[key] = quartic[key] + jnp.sum(q.reshape(-1, ROWS, slots), axis=0)
        for y, z in keys:
            filled = ext[x + 1, y + 1, z0 + z + 1][0:1] < 2.0
            first = jnp.sum(rho[y, z], axis=0, keepdims=True) - 1.0
            second = jnp.sum(quartic[y, z], axis=0, keepdims=True) - 1.0
            first = jnp.where(filled, first, 0.0)
            pair_sum = PAIR_SCALE * (second - 2.0 * first)
            energy = -EMBED_SCALE * jnp.sqrt(first + 1.0) + 0.5 * pair_sum
            energy_ref[x, y, pl.ds(z0 + z, 1)] = jnp.where(filled, energy, 0.0)
            fprime = -0.5 * EMBED_SCALE * lax.rsqrt(first + 1.0)
            gain = 0.5 - fprime * (0.5 / PAIR_SCALE)
            gain_own[x, y, z0 + z] = gain
            gain_ext[x + 1, y + 1, z0 + z + 1] = gain
        return carry

    lax.fori_loop(0, sizes[0] * steps, density_group, 0)
    def raise_gain(x, y):
        rows = [gain_ext[x, y, z] for z in range(wide[2])]
        rows += [jnp.zeros((1, slots), jnp.float32)] * (-wide[2] % ROWS)
        column[x, y, :, : len(rows)] = jnp.concatenate(rows, axis=0).T

    swap_rims(counts, gain_own, gain_ext, gain_sent, gain_landed, None, looped(raise_gain))

    def force_group(index, carry):
        x, z0 = index // steps, index % steps * depth
        tiles = group_tiles(x, z0)
        packs = group_packs(tiles)
        gains = {(y, z): gain_own[x, y, z0 + z] for y, z in keys}
        total = {key: jnp.zeros((4 * ROWS, slots), jnp.float32) for key in keys}
        for dx, jy, jz, runs in plan:
            rows = turned[x + dx, jy, z0 + jz]
            moments = flat[x + dx, jy, z0 + jz]
            if jz == 0:
                lanes = pltpu.roll(column[x + dx, jy], slots - z0, 1)
            far_gain = jnp.broadcast_to(lanes[:, jz : jz + 1], (slots, slots))
            for flag, targets in runs:
                order, pack = packs[flag]
                start = order[targets[0]] * slots
                pack = pack[:, start : start + len(targets) * slots]
                both = jnp.dot(rows, pack, preferred_element_type=jnp.float32)
                highs, lows = [], []
                for at, key in enumerate(targets):
                    w = jnp.maximum(both[:, at * slots : (at + 1) * slots], 0.0)
                    f = w * ((far_gain + gains[key]) - w * w)
                    high = f.astype(jnp.bfloat16)
                    highs.append(high)
                    lows.append((f - high.astype(jnp.float32)).astype(jnp.bfloat16))
                stacked = jnp.concatenate(
                    [jnp.concatenate(highs, axis=1), jnp.concatenate(lows, axis=1)], axis=0
                )
                part = jnp.dot(moments, stacked, preferred_element_type=jnp.float32)
                for at, key in enumerate(targets):
                    total[key] = total[key] + part[:, at * slots : (at + 1) * slots]
        scale = FORCE_SCALE * 4.0 * PAIR_SCALE
        for y, z in keys:
            parts = total[y, z]
            whole = parts[:ROWS] + parts[ROWS : 2 * ROWS] + parts[2 * ROWS : 3 * ROWS]
            filled = ext[x + 1, y + 1, z0 + z + 1][0:1] < 2.0
            push = scale * (whole - 0.125 * tiles[y, z] * whole[4:5])
            push = jnp.where(filled, push, 0.0)
            for component in range(3):
                force_ref[component, x, y, pl.ds(z0 + z, 1)] = push[component : component + 1]
        return carry

    lax.fori_loop(0, sizes[0] * steps, force_group, 0)


def per_device(mesh_counts, positions, counts):
    slots = positions.shape[-1]
    sizes = positions.shape[1:4]
    wide = tuple(size + 2 for size in sizes)
    occupied = jnp.arange(slots, dtype=jnp.int32) < counts[..., None]
    seated = jnp.where(occupied[None], positions, SENTINEL)
    source = jnp.stack([seated[0], seated[1], seated[2], jnp.zeros_like(seated[0])], axis=3)
    return pl.pallas_call(
        functools.partial(kernel, mesh_counts),
        out_shape=(
            jax.ShapeDtypeStruct(sizes + (slots,), jnp.float32),
            jax.ShapeDtypeStruct((3,) + sizes + (slots,), jnp.float32),
        ),
        in_specs=[pl.BlockSpec(memory_space=pltpu.VMEM)],
        out_specs=(pl.BlockSpec(memory_space=pltpu.VMEM),) * 2,
        scratch_shapes=[
            pltpu.VMEM(wide + (4, slots), jnp.float32),
            pltpu.VMEM(sizes + (1, slots), jnp.float32),
            pltpu.VMEM(wide + (1, slots), jnp.float32),
            pltpu.VMEM(wide + (slots, 6 * ROWS), jnp.bfloat16),
            pltpu.VMEM(wide + (4 * ROWS, 2 * slots), jnp.bfloat16),
            pltpu.VMEM(wide[:2] + (slots, slots), jnp.float32),
        ]
        + [pltpu.SemaphoreType.DMA((MESSAGES,))] * 4
        + [pltpu.SemaphoreType.DMA((1,))],
        compiler_params=pltpu.CompilerParams(collective_id=0, has_side_effects=True),
        name="atoms",
    )(source)


def solution(mesh):
    placed = (P(None, "gx", "gy", "gz", None), P("gx", "gy", "gz"))
    return jax.shard_map(
        functools.partial(per_device, tuple(mesh.shape[name] for name in NAMES)),
        mesh=mesh,
        in_specs=placed,
        out_specs=(P("gx", "gy", "gz", None), P(None, "gx", "gy", "gz", None)),
        check_vma=False,
    )
```

```python
import functools

import jax
import jax.numpy as jnp
from jax import lax
from jax.experimental import pallas as pl
from jax.experimental.pallas import tpu as pltpu
from jax.sharding import PartitionSpec as P

SENTINEL = 4.0
PAIR_SCALE = 0.02
EMBED_SCALE = 0.2
CUTOFF_SQUARED = 0.25
FORCE_SCALE = 8.0
FAR = -1.0e6
ROWS = 8


def split(value):
    first = value.astype(jnp.bfloat16).astype(jnp.float32)
    rest = value - first
    second = rest.astype(jnp.bfloat16).astype(jnp.float32)
    return first, second, rest - second


def far_rows(tile):
    b1, b2, b3 = split(tile)
    return jnp.concatenate([b1, b2, b1, b2, b3, b1], axis=0)


def own_rows(tile):
    a1, a2, a3 = split(tile)
    return jnp.concatenate([a1, a1, a2, a2, a1, a3], axis=0)


def place(index, sizes):
    return index // (sizes[1] * sizes[2]), index // sizes[2] % sizes[1], index % sizes[2]


def groups(sizes):
    depth = 2 if sizes[2] % 2 == 0 else 1
    plan = []
    for dx in range(3):
        for jy in range(sizes[1] + 2):
            for jz in range(depth + 2):
                ys = [y for y in range(sizes[1]) if 0 <= jy - y <= 2]
                zs = [z for z in range(depth) if 0 <= jz - z <= 2]
                if len(ys) == sizes[1]:
                    runs = [(True, [(y, z) for z in zs for y in ys])]
                else:
                    runs = [(False, [(y, z) for z in zs]) for y in ys]
                plan.append((dx, jy, jz, runs))
    return depth, plan


def side_by_side(tiles, sizes, depth, layer_first):
    order = (
        [(y, z) for z in range(depth) for y in range(sizes[1])]
        if layer_first
        else [(y, z) for y in range(sizes[1]) for z in range(depth)]
    )
    return {key: at for at, key in enumerate(order)}, jnp.concatenate(
        [tiles[key] for key in order], axis=1
    )


def far_tile(tile, index, wide):
    row = lax.broadcasted_iota(jnp.int32, tile.shape, 0)
    steps = [at.astype(jnp.float32) - 0.5 * size for at, size in zip(index, wide)]
    shift = jnp.where(row == 0, steps[0], jnp.where(row == 1, steps[1], steps[2]))
    filled = tile[0:1] < 2.0
    coords = jnp.where(filled & (row < 3), tile + shift, 0.0)
    near = -4.0 * jnp.sum(coords * coords, axis=0, keepdims=True)
    upper = jnp.where(row == 3, jnp.where(filled, near, FAR), coords)
    lower = jnp.where(row == 0, 1.0, 0.0)
    return jnp.concatenate([upper, lower], axis=0)


def own_tile(tile, index, wide):
    row = lax.broadcasted_iota(jnp.int32, tile.shape, 0)
    far = far_tile(tile, index, wide)
    coords = jnp.where(row < 3, far[:4], 0.0)
    near = 4.0 * jnp.sum(coords * coords, axis=0, keepdims=True)
    upper = jnp.where(row == 3, 1.0, 8.0 * coords)
    lower = jnp.where(row == 0, 1.0 - near, 0.0)
    return jnp.concatenate([upper, lower], axis=0)


NAMES = ("gx", "gy", "gz")
DIRECTIONS = [
    (x, y, z) for x in (-1, 0, 1) for y in (-1, 0, 1) for z in (-1, 0, 1) if (x, y, z) != (0, 0, 0)
]
DIRECTIONS.sort(key=lambda step: -sum(abs(o) for o in step))


def device_at(counts, step):
    return {
        name: lax.rem(lax.axis_index(name) + (offset + count), count)
        for name, offset, count in zip(NAMES, step, counts)
    }


def meet(counts):
    barrier = pltpu.get_barrier_semaphore()
    partners = sorted({tuple(o % c for o, c in zip(step, counts)) for step in DIRECTIONS})
    for step in partners:
        pl.semaphore_signal(
            barrier,
            inc=1,
            device_id=device_at(counts, step),
            device_id_type=pl.DeviceIdType.MESH,
        )
    pl.semaphore_wait(barrier, len(partners))


def send_rims(counts, source, target, sent, landed):
    sizes = source.shape[:3]
    copies = []
    for at, step in enumerate(DIRECTIONS):
        here = tuple(
            pl.ds(0, size) if o == 0 else pl.ds(size - 1 if o > 0 else 0, 1)
            for o, size in zip(step, sizes)
        )
        there = tuple(
            pl.ds(1, size) if o == 0 else pl.ds(0 if o > 0 else size + 1, 1)
            for o, size in zip(step, sizes)
        )
        copy = pltpu.make_async_remote_copy(
            src_ref=source.at[here],
            dst_ref=target.at[there],
            send_sem=sent.at[at],
            recv_sem=landed.at[at],
            device_id=device_at(counts, step),
            device_id_type=pl.DeviceIdType.MESH,
        )
        copy.start()
        copies.append(copy)
    return copies


def drain(copies, sizes, column_work):
    def arrive(chosen):
        for step, copy in zip(DIRECTIONS, copies):
            if chosen(step):
                copy.wait()

    arrive(lambda step: step[:2] == (0, 0))
    column_work(sizes[0] * sizes[1], lambda i: (i // sizes[1] + 1, i % sizes[1] + 1))
    arrive(lambda step: step[0] == 0 and step[1] != 0)
    column_work(2 * sizes[0], lambda i: (i // 2 + 1, i % 2 * (sizes[1] + 1)))
    arrive(lambda step: step[0] != 0 and step[1] == 0)
    column_work(2 * sizes[1], lambda i: (i % 2 * (sizes[0] + 1), i // 2 + 1))
    arrive(lambda step: step[0] != 0 and step[1] != 0)
    column_work(4, lambda i: (i % 2 * (sizes[0] + 1), i // 2 * (sizes[1] + 1)))


def kernel(
    counts,
    source,
    energy_ref,
    force_ref,
    ext,
    gain_own,
    gain_ext,
    turned,
    flat,
    column,
    sent,
    landed,
    gain_sent,
    gain_landed,
):
    sizes = source.shape[:3]
    wide = ext.shape[:3]
    slots = source.shape[-1]
    depth, plan = groups(sizes)
    keys = [(y, z) for y in range(sizes[1]) for z in range(depth)]
    steps = sizes[2] // depth

    meet(counts)
    copies = send_rims(counts, source, ext, sent, landed)

    inner = tuple(slice(1, 1 + size) for size in sizes)
    ext[inner] = source[...]

    def prepare(x, y):
        for z in range(wide[2]):
            b1, b2, b3 = split(far_tile(ext[x, y, z], (x, y, jnp.int32(z)), wide))
            across = jnp.concatenate([b1, b2, b1, b2, b3, b1], axis=0).T
            turned[x, y, z] = across.astype(jnp.bfloat16)
            rows = jnp.concatenate([b1, b2, b3, jnp.zeros_like(b1)], axis=0).astype(jnp.bfloat16)
            flat[x, y, z] = jnp.concatenate([rows, rows], axis=1)

    def looped(body):
        def work(count, where):
            def step(index, carry):
                body(*where(index))
                return carry

            lax.fori_loop(0, count, step, 0)

        return work

    drain(copies, sizes, looped(prepare))

    def group_tiles(x, z0):
        return {
            (y, z): own_tile(ext[x + 1, y + 1, z0 + z + 1], (x + 1, jnp.int32(y + 1), z0 + z + 1), wide)
            for y, z in keys
        }

    def group_packs(tiles):
        rows = {key: own_rows(tile).astype(jnp.bfloat16) for key, tile in tiles.items()}
        return {flag: side_by_side(rows, sizes, depth, flag) for flag in (True, False)}

    def density_group(index, carry):
        x, z0 = index // steps, index % steps * depth
        packs = group_packs(group_tiles(x, z0))
        rho = {key: jnp.zeros((ROWS, slots), jnp.float32) for key in keys}
        quartic = {key: jnp.zeros((ROWS, slots), jnp.float32) for key in keys}
        for dx, jy, jz, runs in plan:
            rows = turned[x + dx, jy, z0 + jz]
            for flag, targets in runs:
                order, pack = packs[flag]
                start = order[targets[0]] * slots
                pack = pack[:, start : start + len(targets) * slots]
                both = jnp.dot(rows, pack, preferred_element_type=jnp.float32)
                for at, key in enumerate(targets):
                    w = jnp.maximum(both[:, at * slots : (at + 1) * slots], 0.0)
                    s = w * w
                    q = s * s
                    rho[key] = rho[key] + jnp.sum(s.reshape(-1, ROWS, slots), axis=0)
                    quartic[key] = quartic[key] + jnp.sum(q.reshape(-1, ROWS, slots), axis=0)
        for y, z in keys:
            filled = ext[x + 1, y + 1, z0 + z + 1][0:1] < 2.0
            first = jnp.sum(rho[y, z], axis=0, keepdims=True) - 1.0
            second = jnp.sum(quartic[y, z], axis=0, keepdims=True) - 1.0
            first = jnp.where(filled, first, 0.0)
            pair_sum = PAIR_SCALE * (second - 2.0 * first)
            energy = -EMBED_SCALE * jnp.sqrt(first + 1.0) + 0.5 * pair_sum
            energy_ref[x, y, pl.ds(z0 + z, 1)] = jnp.where(filled, energy, 0.0)
            fprime = -0.5 * EMBED_SCALE * lax.rsqrt(first + 1.0)
            gain = 0.5 - fprime * (0.5 / PAIR_SCALE)
            gain_own[x, y, z0 + z] = gain
            gain_ext[x + 1, y + 1, z0 + z + 1] = gain
        return carry

    lax.fori_loop(0, sizes[0] * steps, density_group, 0)
    copies = send_rims(counts, gain_own, gain_ext, gain_sent, gain_landed)

    def raise_gain(x, y):
        rows = [gain_ext[x, y, z] for z in range(wide[2])]
        rows += [jnp.zeros((1, slots), jnp.float32)] * (-wide[2] % ROWS)
        column[x, y, :, : len(rows)] = jnp.concatenate(rows, axis=0).T

    drain(copies, sizes, looped(raise_gain))

    def force_group(index, carry):
        x, z0 = index // steps, index % steps * depth
        tiles = group_tiles(x, z0)
        packs = group_packs(tiles)
        gains = {(y, z): gain_own[x, y, z0 + z] for y, z in keys}
        total = {key: jnp.zeros((4 * ROWS, slots), jnp.float32) for key in keys}
        for dx, jy, jz, runs in plan:
            rows = turned[x + dx, jy, z0 + jz]
            moments = flat[x + dx, jy, z0 + jz]
            if jz == 0:
                lanes = pltpu.roll(column[x + dx, jy], slots - z0, 1)
            far_gain = jnp.broadcast_to(lanes[:, jz : jz + 1], (slots, slots))
            for flag, targets in runs:
                order, pack = packs[flag]
                start = order[targets[0]] * slots
                pack = pack[:, start : start + len(targets) * slots]
                both = jnp.dot(rows, pack, preferred_element_type=jnp.float32)
                highs, lows = [], []
                for at, key in enumerate(targets):
                    w = jnp.maximum(both[:, at * slots : (at + 1) * slots], 0.0)
                    f = w * ((far_gain + gains[key]) - w * w)
                    high = f.astype(jnp.bfloat16)
                    highs.append(high)
                    lows.append((f - high.astype(jnp.float32)).astype(jnp.bfloat16))
                stacked = jnp.concatenate(
                    [jnp.concatenate(highs, axis=1), jnp.concatenate(lows, axis=1)], axis=0
                )
                part = jnp.dot(moments, stacked, preferred_element_type=jnp.float32)
                for at, key in enumerate(targets):
                    total[key] = total[key] + part[:, at * slots : (at + 1) * slots]
        scale = FORCE_SCALE * 4.0 * PAIR_SCALE
        for y, z in keys:
            parts = total[y, z]
            whole = parts[:ROWS] + parts[ROWS : 2 * ROWS] + parts[2 * ROWS : 3 * ROWS]
            filled = ext[x + 1, y + 1, z0 + z + 1][0:1] < 2.0
            push = scale * (whole - 0.125 * tiles[y, z] * whole[4:5])
            push = jnp.where(filled, push, 0.0)
            for component in range(3):
                force_ref[component, x, y, pl.ds(z0 + z, 1)] = push[component : component + 1]
        return carry

    lax.fori_loop(0, sizes[0] * steps, force_group, 0)


def per_device(mesh_counts, positions, counts):
    slots = positions.shape[-1]
    sizes = positions.shape[1:4]
    wide = tuple(size + 2 for size in sizes)
    occupied = jnp.arange(slots, dtype=jnp.int32) < counts[..., None]
    seated = jnp.where(occupied[None], positions, SENTINEL)
    source = jnp.stack([seated[0], seated[1], seated[2], jnp.zeros_like(seated[0])], axis=3)
    return pl.pallas_call(
        functools.partial(kernel, mesh_counts),
        out_shape=(
            jax.ShapeDtypeStruct(sizes + (slots,), jnp.float32),
            jax.ShapeDtypeStruct((3,) + sizes + (slots,), jnp.float32),
        ),
        in_specs=[pl.BlockSpec(memory_space=pltpu.VMEM)],
        out_specs=(pl.BlockSpec(memory_space=pltpu.VMEM),) * 2,
        scratch_shapes=[
            pltpu.VMEM(wide + (4, slots), jnp.float32),
            pltpu.VMEM(sizes + (1, slots), jnp.float32),
            pltpu.VMEM(wide + (1, slots), jnp.float32),
            pltpu.VMEM(wide + (slots, 6 * ROWS), jnp.bfloat16),
            pltpu.VMEM(wide + (4 * ROWS, 2 * slots), jnp.bfloat16),
            pltpu.VMEM(wide[:2] + (slots, slots), jnp.float32),
        ]
        + [pltpu.SemaphoreType.DMA((len(DIRECTIONS),))] * 4,
        compiler_params=pltpu.CompilerParams(collective_id=0, has_side_effects=True),
        name="atoms",
    )(source)


def solution(mesh):
    placed = (P(None, "gx", "gy", "gz", None), P("gx", "gy", "gz"))
    return jax.shard_map(
        functools.partial(per_device, tuple(mesh.shape[name] for name in NAMES)),
        mesh=mesh,
        in_specs=placed,
        out_specs=(P("gx", "gy", "gz", None), P(None, "gx", "gy", "gz", None)),
        check_vma=False,
    )
```
